512 devices in a mesh: group: 2 (over y), tm: 32 (over z), space: 4 (over x), head: 2 (over core).
Axes of the slice: x: 4, y: 2, z: 32, core: 2. Of those that a mesh axis runs over, the one named last changes fastest.
The devices are a block of a 4x16x32 slice.
Arguments:
- queries: bfloat16 [64, 32, 32, 3072], P(('group', 'tm'), 'space', None, 'head'), parts along dimension 0, may hold values from -5.5 to 5.5
- keys: bfloat16 [64, 32, 32, 3072], P(('group', 'tm'), 'space', None, 'head'), parts along dimension 0, may hold values from -5.5 to 5.5
- values: bfloat16 [64, 32, 32, 3072], P(('group', 'tm'), 'space', None, 'head'), parts along dimension 0, may hold values from -6 to 6
- window: int32 [64, 4, 4, 27], P(('group', 'tm'), 'space'), parts along dimension 0, may hold values 0 or 1
Outputs:
- attended: bfloat16 [64, 32, 32, 3072], P(('group', 'tm'), 'space', None, 'head'), parts along dimension 0
The draws below stay inside these ranges and needn't reach their ends.
There are 2 independent parts, one for each index of `group`. The reference program is written for one: setup_inputs(seed, part) draws one part's arguments, and reference() takes and returns one part's arrays. A program takes and returns all parts, laid end to end along the dimension named above; each array names one. Nothing has to cross between parts.
Inputs may be any that keep to these rules, and one draw needn't show every extreme that they name: `window`: slot dt * 9 + (dy + 1) * 3 + (dx + 1) of a query tile's entry enables the key tile dt frames earlier, dy tile rows and dx tile columns away; slot 4, the tile itself, is attended whatever it holds.
All inputs are finite; a program needn't handle non-finite values. No bound on the sum of `window` on one device may be relied on, other than what follows from the above.
Results may differ from the reference program's by a relative error of at most 0.0046.
Values may be sent and summed in bfloat16 or wider, within the bound.
No kernel may reach another device: no remote copies, remote signals or barrier semaphores. Data moves between devices by JAX's collectives and lax.ppermute only.
A program may use at most 128 MiB of HBM per device.

```python
import jax
import jax.numpy as jnp
from jax import lax

HEADS = 24
HDIM = 128
TILE = 8
TCOLS = 4
FRAMES = 32
TROWS = 4
ROWS = 32
COLS = 32


def base_field(key, salt):
    shape = (FRAMES, ROWS, COLS, HEADS * HDIM)
    local_key = jax.random.fold_in(key, salt)
    return jnp.clip(jax.random.normal(local_key, shape, jnp.float32), -4.0, 4.0)


def draw_queries(key, part):
    base = base_field(key, 1)
    return base.astype(jnp.bfloat16)


def draw_keys(key, part):
    base = base_field(key, 2)
    return base.astype(jnp.bfloat16)


def plant(entries, rng, smallest, high):
    shape = entries.shape
    index_at = [jax.random.randint(jax.random.fold_in(rng, axis), (), 0, shape[axis]) for axis in range(len(shape))]
    entries = entries.at[tuple(index_at)].set(smallest)
    longest = shape.index(max(shape))
    index_at[longest] = (index_at[longest] + 1) % shape[longest]
    return entries.at[tuple(index_at)].set(high)


def shard_levels(stream_key, dims, split, low, top_value):
    loudness, own = 1.0, jax.random.fold_in(stream_key, 6)
    for dim, shards_of in split:
        draws = jnp.exp(jax.random.uniform(jax.random.fold_in(own, dim), (shards_of,), jnp.float32, low / len(split), top_value / len(split)))
        loudness = loudness * jnp.repeat(draws, dims[dim] // shards_of).reshape([-1 if axis == dim else 1 for axis in range(len(dims))])
    return loudness


def bell_draw(key, extent, deviation, limit, shards=(), held_as=jnp.bfloat16):
    level = shard_levels(key, extent, shards, -0.22, 0.18) if shards else 1.0
    entries = jax.random.normal(key, extent, jnp.float32) * deviation * level
    return jnp.minimum(jnp.maximum(entries, -limit), limit).astype(held_as)


def setup_inputs(seed: int = 0, part: int = 0) -> dict:
    key_list = jax.random.split(jax.random.key(seed), 5)
    own_keys = jax.random.split(jax.random.fold_in(key_list[4], part), 5)
    return {
        "queries": draw_queries(jax.random.fold_in(jax.random.fold_in(key_list[4], part), 71), part),
        "keys": draw_keys(jax.random.fold_in(jax.random.fold_in(key_list[4], part), 71), part),
        "values": bell_draw(own_keys[2], (FRAMES, ROWS, COLS, HEADS * HDIM), 1.0, 6.0, ((0, 32), (1, 4), (3, 2))),
        "window": plant((jax.random.randint(own_keys[3], (FRAMES, TROWS, TCOLS, 27), 0, 3) < 2).astype(jnp.int32), jax.random.fold_in(own_keys[3], 1), 0, 1),
    }


def reference(queries, keys, values, window):
    channels = HEADS * HDIM
    pad_spec = ((2, 0), (TILE, TILE), (TILE, TILE), (0, 0))
    keys_padded = jnp.pad(keys, pad_spec)
    values_padded = jnp.pad(values, pad_spec)
    score_scale = HDIM ** -0.5
    steps_back = jnp.arange(3, dtype=jnp.int32)
    shifts = jnp.arange(3, dtype=jnp.int32) - 1
    slot_of = steps_back[:, None, None] * 9 + (shifts[None, :, None] + 1) * 3 + shifts[None, None, :] + 1
    slot_ids = jnp.arange(27, dtype=jnp.int32)
    zero_idx = jnp.int32(0)

    def attend(tile_id):
        frame = tile_id // (TROWS * TCOLS)
        tile_row = (tile_id // TCOLS) % TROWS
        tile_col = tile_id % TCOLS
        query_tile = lax.dynamic_slice(queries, (frame, tile_row * TILE, tile_col * TILE, zero_idx), (1, TILE, TILE, channels))
        query_tile = query_tile.reshape(TILE * TILE, HEADS, HDIM).astype(jnp.float32)
        key_block = lax.dynamic_slice(keys_padded, (frame, tile_row * TILE, tile_col * TILE, zero_idx), (3, 3 * TILE, 3 * TILE, channels))[::-1]
        value_block = lax.dynamic_slice(values_padded, (frame, tile_row * TILE, tile_col * TILE, zero_idx), (3, 3 * TILE, 3 * TILE, channels))[::-1]
        key_rows = key_block.reshape(27 * TILE * TILE, HEADS, HDIM).astype(jnp.float32)
        value_rows = value_block.reshape(27 * TILE * TILE, HEADS, HDIM).astype(jnp.float32)
        frame_ok = frame - steps_back >= 0
        row_ok = (tile_row + shifts >= 0) & (tile_row + shifts < TROWS)
        col_ok = (tile_col + shifts >= 0) & (tile_col + shifts < TCOLS)
        bits_row = lax.dynamic_slice(window, (frame, tile_row, tile_col, zero_idx), (1, 1, 1, 27)).reshape(27)
        picked = jnp.sum(jnp.where(slot_of[..., None] == slot_ids, bits_row, 0), axis=-1)
        allowed = ((picked == 1) | (slot_of == 4)) & frame_ok[:, None, None] & row_ok[None, :, None] & col_ok[None, None, :]
        key_ok = jnp.broadcast_to(allowed[:, :, None, :, None], (3, 3, TILE, 3, TILE)).reshape(27 * TILE * TILE)
        scores = jnp.einsum("qhd,khd->hqk", query_tile, key_rows) * score_scale
        scores = jnp.where(key_ok, scores, -jnp.inf)
        row_max = jnp.max(scores, axis=-1, keepdims=True)
        weights = jnp.exp(scores - row_max)
        row_sum = jnp.sum(weights, axis=-1)
        weights_bf = lax.optimization_barrier(weights.astype(jnp.bfloat16)).astype(jnp.float32)
        numerator = jnp.einsum("hqk,khd->qhd", weights_bf, value_rows)
        result = numerator / row_sum.T[:, :, None]
        return result.astype(jnp.bfloat16).reshape(TILE, TILE, channels)

    per_tile = lax.map(attend, jnp.arange(FRAMES * TROWS * TCOLS, dtype=jnp.int32))
    per_tile = per_tile.reshape(FRAMES, TROWS, TCOLS, TILE, TILE, channels)
    return per_tile.transpose(0, 1, 3, 2, 4, 5).reshape(FRAMES, ROWS, COLS, channels)
```

```python
import functools

import jax
import jax.numpy as jnp
from jax import lax
from jax.experimental import pallas as pl
from jax.experimental.pallas import tpu as pltpu
from jax.sharding import PartitionSpec as P


HDIM = 128
TILE = 8
SLOTS = 27
MASKS = 48
STATS = 8
NEVER = -1e30
FLOOR = -1e25
SCALE = (HDIM**-0.5) * 1.4426950408889634
WHOLE = pl.BlockSpec(memory_space=pltpu.VMEM)
ROW_BEFORE, ROW_AFTER, FRAME_1, FRAME_2 = range(4)
LAG = 6


def shift(block, axis, by, skip=0, ahead=0):
    size = lax.axis_size(axis)
    route = [
        (i, i + by)
        for i in range(skip, size)
        if 0 <= i + by < size and i + by + ahead < size and i + ahead < size
    ]
    return lax.ppermute(block, axis, route)


def masks(tcols, flags, window):
    row = lax.broadcasted_iota(jnp.int32, (MASKS, HDIM), 0)
    lane = lax.broadcasted_iota(jnp.int32, (MASKS, HDIM), 1)
    place, key_tile = lax.div(row, tcols), lax.rem(row, tcols)
    total = jnp.zeros((MASKS, HDIM), jnp.float32)
    for c in range(tcols):
        bits = jnp.broadcast_to(window[c : c + 1, :], (MASKS, SLOTS))
        bits = jnp.concatenate([bits, jnp.zeros((MASKS, HDIM - SLOTS), jnp.float32)], axis=1)
        step = key_tile - c
        bits = jnp.where((lane == place * 3 + step + 1) & (jnp.abs(step) <= 1), bits, 0.0)
        total = jnp.where(lane == c, jnp.sum(bits, axis=1, keepdims=True), total)
    own = (place == 1) & (key_tile == lane)
    back, dy = lax.div(place, 3), lax.rem(place, 3)
    ok = jnp.full((MASKS, HDIM), 1, jnp.int32)
    ok = jnp.where(dy == 0, flags[ROW_BEFORE], ok)
    ok = jnp.where(dy == 2, flags[ROW_AFTER], ok)
    ok = jnp.where(back == 1, ok * flags[FRAME_1], ok)
    ok = jnp.where(back == 2, ok * flags[FRAME_2], ok)
    allowed = ((total > 0.5) | own) & (ok > 0)
    return jnp.where(allowed | (lane >= tcols), 0.0, NEVER).astype(jnp.bfloat16)


def pack_kernel(heads, tokens, q_ref, k_ref, v_ref, w_ref, *refs):
    packed, ok_ref, (vbuf, wbuf, sems) = refs[:4], refs[4], refs[5:]
    table = pltpu.make_async_copy(w_ref.at[0, 0], wbuf, sems.at[6 * heads])
    table.start()
    rows, cols = q_ref.shape[1], q_ref.shape[2]
    copies = {}
    for half in range(2):
        qc_ref, kv_ref = packed[2 * half : 2 * half + 2]
        for j in range(heads):
            head = half * heads + j
            lanes = pl.ds(head * HDIM, HDIM)
            at = pl.ds(j * tokens, tokens)
            slot = pl.ds(head * tokens, tokens)
            for n, (src, dst) in enumerate(
                ((v_ref, vbuf.at[slot]), (k_ref, kv_ref.at[at]), (q_ref, qc_ref.at[at]))
            ):
                copy = pltpu.make_async_copy(
                    src.at[0, :, :, lanes],
                    dst.reshape(rows, cols, HDIM),
                    sems.at[3 * head + n],
                )
                copy.start()
                copies[half, j, n] = copy
    here, frame = lax.axis_index("space"), lax.axis_index("tm")
    tests = here > 0, here < lax.axis_size("space") - 1, frame > 0, frame > 1
    flags = [jnp.where(test, 1, 0) for test in tests]
    sub = lax.broadcasted_iota(jnp.int32, ok_ref.shape, 0)
    ok = jnp.zeros(ok_ref.shape, jnp.int32)
    for n, flag in enumerate(flags):
        ok = jnp.where(sub == n, flag, ok)
    ok_ref[...] = ok
    table.wait()
    mask = masks(cols // TILE, flags, wbuf[...].astype(jnp.float32))
    for half in range(2):
        qc_ref, kv_ref = packed[2 * half : 2 * half + 2]
        qc_ref[heads * tokens :, :] = mask
        for j in range(heads):
            copies[half, j, 0].wait()
            slot = (half * heads + j) * tokens
            vt = vbuf[slot : slot + tokens, :].T
            base = (heads + j) * tokens
            for s in range(tokens // HDIM):
                kv_ref[base + s * HDIM : base + (s + 1) * HDIM, :] = vt[
                    :, s * HDIM : (s + 1) * HDIM
                ]
    for half in range(2):
        for j in range(heads):
            copies[half, j, 1].wait()
            copies[half, j, 2].wait()


def pack(heads, queries, keys, values, window):
    tokens = queries.shape[1] * queries.shape[2]
    shapes = [
        jax.ShapeDtypeStruct((heads * tokens + MASKS, HDIM), jnp.bfloat16),
        jax.ShapeDtypeStruct((2 * heads * tokens, HDIM), jnp.bfloat16),
    ]
    return pl.pallas_call(
        functools.partial(pack_kernel, heads, tokens),
        out_shape=shapes * 2 + [jax.ShapeDtypeStruct((STATS, HDIM), jnp.int32)],
        in_specs=[pl.BlockSpec(memory_space=pltpu.HBM)] * 4,
        out_specs=[WHOLE] * 5,
        scratch_shapes=[
            pltpu.VMEM((2 * heads * tokens, HDIM), jnp.bfloat16),
            pltpu.VMEM(window.shape[2:], window.dtype),
            pltpu.SemaphoreType.DMA((6 * heads + 1,)),
        ],
        compiler_params=pltpu.CompilerParams(vmem_limit_bytes=8 * 2**20),
        cost_estimate=pl.CostEstimate(
            flops=10**9, bytes_accessed=12 * heads * tokens * HDIM, transcendentals=0
        ),
        name="pack",
    )(queries, keys, values, window)


def side_by_side(ref, base, tokens):
    return jnp.concatenate(
        [ref[base + s * HDIM : base + (s + 1) * HDIM, :] for s in range(tokens // HDIM)], axis=1
    )


def write_partial(out_ref, heads, tokens, outs, lse):
    halves = tokens // HDIM
    for j, out in outs:
        for s in range(halves):
            at = j * tokens + s * HDIM
            out_ref[at : at + HDIM, :] = out[:, s * HDIM : (s + 1) * HDIM]
    if lse is not None:
        for p in range(3):
            part = lse.astype(jnp.bfloat16)
            lse = lse - part.astype(jnp.float32)
            for s in range(halves):
                at = heads * tokens + (p * halves + s) * STATS
                out_ref[at : at + STATS, :] = part[:, s * HDIM : (s + 1) * HDIM]


def read_lse(in_ref, heads, tokens):
    halves = tokens // HDIM
    parts = []
    for s in range(halves):
        part = jnp.zeros((STATS, HDIM), jnp.float32)
        for p in range(3):
            at = heads * tokens + (p * halves + s) * STATS
            part = part + in_ref[at : at + STATS, :].astype(jnp.float32)
        parts.append(part)
    return jnp.concatenate(parts, axis=1)


def attend_kernel(heads, tokens, cols, sets, packed, *refs):
    q_refs, refs = refs[: len(sets)], refs[len(sets) :]
    blocks = len(sets[0])
    kvs, refs = refs[:blocks], refs[blocks:]
    tcols = cols // TILE
    repeat = tokens // cols

    row = lax.broadcasted_iota(jnp.int32, (cols, HDIM), 0)
    lane = lax.broadcasted_iota(jnp.int32, (cols, HDIM), 1)
    tile = jnp.where(lane == lax.div(row, TILE), 1.0, 0.0).astype(jnp.bfloat16)
    tile = jnp.concatenate([tile] * repeat, axis=0)
    bias = {}
    for which, places in enumerate(sets):
        rows = q_refs[which][heads * tokens :, :].astype(jnp.float32)
        for n, place in enumerate(places):
            part = [
                jnp.broadcast_to(rows[place * tcols + c : place * tcols + c + 1, :], (TILE, HDIM))
                for c in range(tcols)
            ]
            part = jnp.concatenate(part, axis=0).astype(jnp.bfloat16)
            bias[which, n] = jnp.concatenate([part] * repeat, axis=0)

    streams = [(which, j) for which in range(len(sets)) for j in range(heads)]
    group = 3 if len(streams) % 3 == 0 else 1
    units = [
        (n, stream)
        for base in range(0, len(streams), group)
        for n in range(blocks)
        for stream in streams[base : base + group]
    ]
    tops, totals, outs, ready = {}, {}, {}, {}
    sub = lax.broadcasted_iota(jnp.int32, (STATS, tokens), 0)
    lses = [jnp.full((STATS, tokens), NEVER, jnp.float32) for _ in sets]
    for i in range(len(units) + LAG):
        if i < len(units):
            n, key = units[i]
            which, j = key
            at = slice(j * tokens, (j + 1) * tokens)
            qcat = jnp.concatenate([q_refs[which][at, :], tile], axis=1)
            kcat = jnp.concatenate([kvs[n][at, :], bias[which, n]], axis=1)
            scores = lax.dot_general(
                kcat, qcat, (((1,), (1,)), ((), ())), preferred_element_type=jnp.float32
            )
            top = jnp.max(scores, axis=0, keepdims=True) * SCALE
            old = tops.get(key)
            top = jnp.maximum(top, FLOOR if old is None else old)
            tops[key] = top
            weights = jnp.exp2(scores * SCALE - top)
            total = jnp.sum(weights, axis=0, keepdims=True)
            fade = None if old is None else jnp.exp2(old - top)
            totals[key] = total if old is None else totals[key] * fade + total
            ready[i] = fade, weights.astype(jnp.bfloat16)
        if i >= LAG:
            n, key = units[i - LAG]
            which, j = key
            fade, weights = ready.pop(i - LAG)
            out = jnp.dot(
                side_by_side(kvs[n], (heads + j) * tokens, tokens),
                weights,
                preferred_element_type=jnp.float32,
            )
            outs[key] = out if fade is None else outs[key] * fade + out
            if n == blocks - 1:
                total = totals[key]
                out = outs.pop(key) * (1.0 / jnp.maximum(total, 1e-30))
                lse = tops[key] + jnp.log2(total)
                lses[which] = jnp.where((sub == j) & (total > 0), lse, lses[which])
                if packed[which]:
                    write_partial(
                        refs[which], heads, tokens, [(j, out.astype(jnp.bfloat16))], None
                    )
                else:
                    refs[which][j * HDIM : (j + 1) * HDIM, :] = out
    for which, lse in enumerate(lses):
        if packed[which]:
            write_partial(refs[which], heads, tokens, [], lse)
        else:
            refs[which][heads * HDIM :, :] = lse


def partial_shape(heads, tokens):
    stats = 3 * (tokens // HDIM) * STATS
    return jax.ShapeDtypeStruct((heads * tokens + stats, HDIM), jnp.bfloat16)


def attend(sets, packed, heads, shape, qs, kvs):
    rows, cols, _ = shape
    tokens = rows * cols
    out_shape = [
        partial_shape(heads, tokens)
        if p
        else jax.ShapeDtypeStruct((heads * HDIM + STATS, tokens), jnp.float32)
        for p in packed
    ]
    return pl.pallas_call(
        functools.partial(attend_kernel, heads, tokens, cols, sets, packed),
        out_shape=out_shape,
        in_specs=[WHOLE] * (len(qs) + len(kvs)),
        out_specs=[WHOLE] * len(packed),
        compiler_params=pltpu.CompilerParams(vmem_limit_bytes=16 * 2**20),
        cost_estimate=pl.CostEstimate(
            flops=10**9, bytes_accessed=8 * heads * tokens * HDIM, transcendentals=0
        ),
        name="attend",
    )(*qs, *kvs)


def merged(heads, tokens, ok_ref, local, priors, checks, write):
    lses = [local[heads * HDIM :, :]]
    for ref, flag in zip(priors, checks):
        ok = jnp.concatenate([ok_ref[flag : flag + 1, :]] * (tokens // HDIM), axis=1)
        lses.append(jnp.where(ok > 0, read_lse(ref, heads, tokens), NEVER))
    top = functools.reduce(jnp.maximum, lses)
    shares = [jnp.exp2(lse - top) for lse in lses]
    total = functools.reduce(jnp.add, shares)
    shares = [share * (1.0 / total) for share in shares]
    for j in range(heads):
        out = local[j * HDIM : (j + 1) * HDIM, :] * shares[0][j : j + 1, :]
        for ref, share in zip(priors, shares[1:]):
            piece = side_by_side(ref, j * tokens, tokens).astype(jnp.float32)
            out = out + piece * share[j : j + 1, :]
        write(j, out.astype(jnp.bfloat16))
    return jnp.where(top > 0.5 * NEVER, top + jnp.log2(total), NEVER)


def merge_kernel(heads, tokens, checks, ok_ref, local, *refs):
    priors, out_ref = refs[:-1], refs[-1]

    def write(j, out):
        write_partial(out_ref, heads, tokens, [(j, out)], None)

    lse = merged(heads, tokens, ok_ref, local, priors, checks, write)
    write_partial(out_ref, heads, tokens, [], lse)


def finish_kernel(heads, tokens, cols, parts, ok_ref, *refs):
    out_ref, stage, sems = refs[-3:]
    copies = []
    for first, checks in parts:
        local, priors, refs = refs[0], refs[1 : 1 + len(checks)], refs[1 + len(checks) :]

        def write(j, out):
            at = pl.ds((first + j) * tokens, tokens)
            stage[at, :] = out.T
            copy = pltpu.make_async_copy(
                stage.at[at].reshape(tokens // cols, cols, HDIM),
                out_ref.at[0, :, :, pl.ds((first + j) * HDIM, HDIM)],
                sems.at[first + j],
            )
            copy.start()
            copies.append(copy)

        merged(heads, tokens, ok_ref, local, priors, checks, write)
    for copy in copies:
        copy.wait()


def merge(heads, shape, ok, local, priors, checks):
    tokens = shape[0] * shape[1]
    return pl.pallas_call(
        functools.partial(merge_kernel, heads, tokens, checks),
        out_shape=partial_shape(heads, tokens),
        in_specs=[WHOLE] * (2 + len(priors)),
        out_specs=WHOLE,
        compiler_params=pltpu.CompilerParams(vmem_limit_bytes=8 * 2**20),
        cost_estimate=pl.CostEstimate(
            flops=10**8, bytes_accessed=8 * heads * tokens * HDIM, transcendentals=0
        ),
        name="merge",
    )(ok, local, *priors)


def finish(heads, shape, ok, *parts):
    rows, cols, channels = shape
    tokens = rows * cols
    args = [ok]
    for _, local, priors, _ in parts:
        args += [local, *priors]
    layout = tuple((first, checks) for first, _, _, checks in parts)
    return pl.pallas_call(
        functools.partial(finish_kernel, heads, tokens, cols, layout),
        out_shape=jax.ShapeDtypeStruct((1, rows, cols, channels), jnp.bfloat16),
        in_specs=[WHOLE] * len(args),
        out_specs=pl.BlockSpec(memory_space=pl.ANY),
        scratch_shapes=[
            pltpu.VMEM((tokens * channels // HDIM, HDIM), jnp.bfloat16),
            pltpu.SemaphoreType.DMA((channels // HDIM,)),
        ],
        compiler_params=pltpu.CompilerParams(vmem_limit_bytes=8 * 2**20),
        cost_estimate=pl.CostEstimate(
            flops=10**8, bytes_accessed=16 * heads * tokens * HDIM, transcendentals=0
        ),
        name="finish",
    )(*args)


def steps(queries, keys, values, window):
    _, rows, cols, channels = queries.shape
    args = (
        pltpu.with_memory_space_constraint(a, pltpu.HBM) for a in (queries, keys, values, window)
    )
    half = channels // HDIM // 2
    shape = (rows, cols, channels)
    go = functools.partial(attend, heads=half, shape=shape)
    qa, kva, qb, kvb, ok = pack(half, *args)

    a1 = shift(kva, "tm", 1)
    a2 = shift(a1, "tm", 1, skip=1)
    qm = shift(qa, "space", 1)
    qp = shift(qa, "space", -1)
    along = (kva, a1, a2)
    frames = [tuple(3 * back + dy for back in range(3)) for dy in range(3)]
    both, mine = (True, True), (False,)
    km, kp = go((frames[2], frames[0]), both, qs=(qm, qp), kvs=along)
    pp = shift(km, "space", -1)
    pm = shift(kp, "space", 1)
    (ka,) = go((frames[1],), mine, qs=(qa,), kvs=along)

    q1 = shift(qb, "tm", -1)
    q2 = shift(q1, "tm", -1, ahead=1)
    lo = shift(kvb, "space", 1)
    hi = shift(kvb, "space", -1)
    across = (lo, kvb, hi)
    offsets = [tuple(3 * back + dy for dy in range(3)) for back in range(3)]

    (k2,) = go((offsets[2],), (True,), qs=(q2,), kvs=across)
    p2 = shift(k2, "tm", 1, ahead=1)
    k1, k0 = go((offsets[1], offsets[0]), (False, False), qs=(q1, qb), kvs=across)
    m1 = merge(half, shape, ok, k1, (p2,), (FRAME_1,))
    p1 = shift(m1, "tm", 1)

    part_a = (0, ka, (pm, pp), (ROW_BEFORE, ROW_AFTER))
    part_b = (half, k0, (p1,), (FRAME_1,))
    return finish(half, shape, ok, part_a, part_b)


def solution(mesh):
    arrays = P(("group", "tm"), "space", None, "head")
    return jax.shard_map(
        steps,
        mesh=mesh,
        in_specs=(arrays, arrays, arrays, P(("group", "tm"), "space", None, None)),
        out_specs=arrays,
        check_vma=False,
    )
```

```python
import functools

import jax
import jax.numpy as jnp
from jax import lax
from jax.experimental import pallas as pl
from jax.experimental.pallas import tpu as pltpu
from jax.sharding import PartitionSpec as P


HDIM = 128
TILE = 8
SLOTS = 27
MASKS = 48
STATS = 8
NEVER = -1e30
FLOOR = -1e25
SCALE = (HDIM**-0.5) * 1.4426950408889634
WHOLE = pl.BlockSpec(memory_space=pltpu.VMEM)
ROW_BEFORE, ROW_AFTER, FRAME_1, FRAME_2 = range(4)
LAG = 6


def shift(block, axis, by, skip=0, ahead=0):
    size = lax.axis_size(axis)
    route = [
        (i, i + by)
        for i in range(skip, size)
        if 0 <= i + by < size and i + by + ahead < size and i + ahead < size
    ]
    return lax.ppermute(block, axis, route)


def masks(tcols, flags, window):
    row = lax.broadcasted_iota(jnp.int32, (MASKS, HDIM), 0)
    lane = lax.broadcasted_iota(jnp.int32, (MASKS, HDIM), 1)
    place, key_tile = lax.div(row, tcols), lax.rem(row, tcols)
    total = jnp.zeros((MASKS, HDIM), jnp.float32)
    for c in range(tcols):
        bits = jnp.broadcast_to(window[c : c + 1, :], (MASKS, SLOTS))
        bits = jnp.concatenate([bits, jnp.zeros((MASKS, HDIM - SLOTS), jnp.float32)], axis=1)
        step = key_tile - c
        bits = jnp.where((lane == place * 3 + step + 1) & (jnp.abs(step) <= 1), bits, 0.0)
        total = jnp.where(lane == c, jnp.sum(bits, axis=1, keepdims=True), total)
    own = (place == 1) & (key_tile == lane)
    back, dy = lax.div(place, 3), lax.rem(place, 3)
    ok = jnp.full((MASKS, HDIM), 1, jnp.int32)
    ok = jnp.where(dy == 0, flags[ROW_BEFORE], ok)
    ok = jnp.where(dy == 2, flags[ROW_AFTER], ok)
    ok = jnp.where(back == 1, ok * flags[FRAME_1], ok)
    ok = jnp.where(back == 2, ok * flags[FRAME_2], ok)
    allowed = ((total > 0.5) | own) & (ok > 0)
    return jnp.where(allowed | (lane >= tcols), 0.0, NEVER).astype(jnp.bfloat16)


def pack_kernel(heads, tokens, q_ref, k_ref, v_ref, w_ref, *refs):
    packed, ok_ref, (vbuf, wbuf, sems) = refs[:4], refs[4], refs[5:]
    table = pltpu.make_async_copy(w_ref.at[0, 0], wbuf, sems.at[6 * heads])
    table.start()
    rows, cols = q_ref.shape[1], q_ref.shape[2]
    copies = {}
    for n, src in enumerate((v_ref, k_ref, q_ref)):
        for head in range(2 * heads):
            half, j = divmod(head, heads)
            if n == 0:
                dst = vbuf.at[pl.ds(head * tokens, tokens)]
            else:
                dst = packed[2 * half + n % 2].at[pl.ds(j * tokens, tokens)]
            copy = pltpu.make_async_copy(
                src.at[0, :, :, pl.ds(head * HDIM, HDIM)],
                dst.reshape(rows, cols, HDIM),
                sems.at[3 * head + n],
            )
            copy.start()
            copies[n, head] = copy
    here, frame = lax.axis_index("space"), lax.axis_index("tm")
    tests = here > 0, here < lax.axis_size("space") - 1, frame > 0, frame > 1
    flags = [jnp.where(test, 1, 0) for test in tests]
    sub = lax.broadcasted_iota(jnp.int32, ok_ref.shape, 0)
    ok = jnp.zeros(ok_ref.shape, jnp.int32)
    for n, flag in enumerate(flags):
        ok = jnp.where(sub == n, flag, ok)
    ok_ref[...] = ok
    table.wait()
    mask = masks(cols // TILE, flags, wbuf[...].astype(jnp.float32))
    for half in range(2):
        packed[2 * half][heads * tokens :, :] = mask
    for head in range(2 * heads):
        copies[0, head].wait()
    for head in range(2 * heads):
        half, j = divmod(head, heads)
        vt = vbuf[head * tokens : (head + 1) * tokens, :].T
        for s in range(tokens // HDIM):
            at = (heads + j) * tokens + s * HDIM
            packed[2 * half + 1][at : at + HDIM, :] = vt[:, s * HDIM : (s + 1) * HDIM]
    for head in range(2 * heads):
        copies[1, head].wait()
        copies[2, head].wait()


def pack(heads, queries, keys, values, window):
    tokens = queries.shape[1] * queries.shape[2]
    shapes = [
        jax.ShapeDtypeStruct((heads * tokens + MASKS, HDIM), jnp.bfloat16),
        jax.ShapeDtypeStruct((2 * heads * tokens, HDIM), jnp.bfloat16),
    ]
    return pl.pallas_call(
        functools.partial(pack_kernel, heads, tokens),
        out_shape=shapes * 2 + [jax.ShapeDtypeStruct((STATS, HDIM), jnp.int32)],
        in_specs=[pl.BlockSpec(memory_space=pltpu.HBM)] * 4,
        out_specs=[WHOLE] * 5,
        scratch_shapes=[
            pltpu.VMEM((2 * heads * tokens, HDIM), jnp.bfloat16),
            pltpu.VMEM(window.shape[2:], window.dtype),
            pltpu.SemaphoreType.DMA((6 * heads + 1,)),
        ],
        compiler_params=pltpu.CompilerParams(vmem_limit_bytes=8 * 2**20),
        cost_estimate=pl.CostEstimate(
            flops=10**9, bytes_accessed=12 * heads * tokens * HDIM, transcendentals=0
        ),
        name="pack",
    )(queries, keys, values, window)


def side_by_side(ref, base, tokens):
    return jnp.concatenate(
        [ref[base + s * HDIM : base + (s + 1) * HDIM, :] for s in range(tokens // HDIM)], axis=1
    )


def write_partial(out_ref, heads, tokens, outs, lse):
    halves = tokens // HDIM
    for j, out in outs:
        for s in range(halves):
            at = j * tokens + s * HDIM
            out_ref[at : at + HDIM, :] = out[:, s * HDIM : (s + 1) * HDIM]
    if lse is not None:
        for p in range(3):
            part = lse.astype(jnp.bfloat16)
            lse = lse - part.astype(jnp.float32)
            for s in range(halves):
                at = heads * tokens + (p * halves + s) * STATS
                out_ref[at : at + STATS, :] = part[:, s * HDIM : (s + 1) * HDIM]


def read_lse(in_ref, heads, tokens):
    halves = tokens // HDIM
    parts = []
    for s in range(halves):
        part = jnp.zeros((STATS, HDIM), jnp.float32)
        for p in range(3):
            at = heads * tokens + (p * halves + s) * STATS
            part = part + in_ref[at : at + STATS, :].astype(jnp.float32)
        parts.append(part)
    return jnp.concatenate(parts, axis=1)


def attend_kernel(heads, tokens, cols, sets, packed, cases, *refs):
    q_refs, refs = refs[: len(sets)], refs[len(sets) :]
    blocks = len(sets[0])
    kvs, out_refs = refs[:blocks], refs[blocks:]
    run = functools.partial(attend_case, heads, tokens, cols, sets, packed, q_refs, kvs, out_refs)
    everything = tuple(range(len(sets))), tuple(range(blocks))
    rest = None
    for where, chosen, used in (*cases, ((), *everything)):
        hit = rest
        for axis, index in where:
            same = lax.axis_index(axis) == index % lax.axis_size(axis)
            hit = same if hit is None else hit & same
        if hit is None:
            run(chosen, used)
            return
        pl.when(hit)(functools.partial(run, chosen, used))
        rest = jnp.logical_not(hit) if rest is None else rest & jnp.logical_not(hit)


def attend_case(heads, tokens, cols, sets, packed, q_refs, kvs, out_refs, chosen, used):
    tcols = cols // TILE
    repeat = tokens // cols

    row = lax.broadcasted_iota(jnp.int32, (cols, HDIM), 0)
    lane = lax.broadcasted_iota(jnp.int32, (cols, HDIM), 1)
    tile = jnp.where(lane == lax.div(row, TILE), 1.0, 0.0).astype(jnp.bfloat16)
    tile = jnp.concatenate([tile] * repeat, axis=0)
    bias = {}
    for which in chosen:
        rows = q_refs[which][heads * tokens :, :].astype(jnp.float32)
        for n in used:
            at = sets[which][n] * tcols
            part = [
                jnp.broadcast_to(rows[at + c : at + c + 1, :], (TILE, HDIM)) for c in range(tcols)
            ]
            part = jnp.concatenate(part, axis=0).astype(jnp.bfloat16)
            bias[which, n] = jnp.concatenate([part] * repeat, axis=0)

    streams = [(which, j) for which in chosen for j in range(heads)]
    group = 3 if len(streams) % 3 == 0 else 1
    units = [
        (n, stream)
        for base in range(0, len(streams), group)
        for n in used
        for stream in streams[base : base + group]
    ]
    tops, totals, outs, ready = {}, {}, {}, {}
    sub = lax.broadcasted_iota(jnp.int32, (STATS, tokens), 0)
    lses = {which: jnp.full((STATS, tokens), NEVER, jnp.float32) for which in chosen}
    for i in range(len(units) + LAG):
        if i < len(units):
            n, key = units[i]
            which, j = key
            at = slice(j * tokens, (j + 1) * tokens)
            qcat = jnp.concatenate([q_refs[which][at, :], tile], axis=1)
            kcat = jnp.concatenate([kvs[n][at, :], bias[which, n]], axis=1)
            scores = lax.dot_general(
                kcat, qcat, (((1,), (1,)), ((), ())), preferred_element_type=jnp.float32
            )
            top = jnp.max(scores, axis=0, keepdims=True) * SCALE
            old = tops.get(key)
            top = jnp.maximum(top, FLOOR if old is None else old)
            tops[key] = top
            weights = jnp.exp2(scores * SCALE - top)
            total = jnp.sum(weights, axis=0, keepdims=True)
            fade = None if old is None else jnp.exp2(old - top)
            totals[key] = total if old is None else totals[key] * fade + total
            ready[i] = fade, weights.astype(jnp.bfloat16)
        if i >= LAG:
            n, key = units[i - LAG]
            which, j = key
            fade, weights = ready.pop(i - LAG)
            out = jnp.dot(
                side_by_side(kvs[n], (heads + j) * tokens, tokens),
                weights,
                preferred_element_type=jnp.float32,
            )
            outs[key] = out if fade is None else outs[key] * fade + out
            if n == used[-1]:
                total = totals[key]
                out = outs.pop(key) * (1.0 / jnp.maximum(total, 1e-30))
                lse = tops[key] + jnp.log2(total)
                lses[which] = jnp.where((sub == j) & (total > 0), lse, lses[which])
                if packed[which]:
                    write_partial(
                        out_refs[which], heads, tokens, [(j, out.astype(jnp.bfloat16))], None
                    )
                else:
                    out_refs[which][j * HDIM : (j + 1) * HDIM, :] = out
    for which, lse in lses.items():
        if packed[which]:
            write_partial(out_refs[which], heads, tokens, [], lse)
        else:
            out_refs[which][heads * HDIM :, :] = lse


def partial_shape(heads, tokens):
    stats = 3 * (tokens // HDIM) * STATS
    return jax.ShapeDtypeStruct((heads * tokens + stats, HDIM), jnp.bfloat16)


def attend(sets, packed, cases, heads, shape, qs, kvs):
    rows, cols, _ = shape
    tokens = rows * cols
    out_shape = [
        partial_shape(heads, tokens)
        if p
        else jax.ShapeDtypeStruct((heads * HDIM + STATS, tokens), jnp.float32)
        for p in packed
    ]
    return pl.pallas_call(
        functools.partial(attend_kernel, heads, tokens, cols, sets, packed, cases),
        out_shape=out_shape,
        in_specs=[WHOLE] * (len(qs) + len(kvs)),
        out_specs=[WHOLE] * len(packed),
        compiler_params=pltpu.CompilerParams(vmem_limit_bytes=16 * 2**20),
        cost_estimate=pl.CostEstimate(
            flops=10**9, bytes_accessed=8 * heads * tokens * HDIM, transcendentals=0
        ),
        name="attend",
    )(*qs, *kvs)


def merged(heads, tokens, ok_ref, local, priors, checks, write):
    lses = [local[heads * HDIM :, :]]
    for ref, flag in zip(priors, checks):
        ok = jnp.concatenate([ok_ref[flag : flag + 1, :]] * (tokens // HDIM), axis=1)
        lses.append(jnp.where(ok > 0, read_lse(ref, heads, tokens), NEVER))
    top = functools.reduce(jnp.maximum, lses)
    shares = [jnp.exp2(lse - top) for lse in lses]
    total = functools.reduce(jnp.add, shares)
    shares = [share * (1.0 / total) for share in shares]
    for j in range(heads):
        out = local[j * HDIM : (j + 1) * HDIM, :] * shares[0][j : j + 1, :]
        for ref, share in zip(priors, shares[1:]):
            piece = side_by_side(ref, j * tokens, tokens).astype(jnp.float32)
            out = out + piece * share[j : j + 1, :]
        write(j, out.astype(jnp.bfloat16))
    return jnp.where(top > 0.5 * NEVER, top + jnp.log2(total), NEVER)


def merge_kernel(heads, tokens, checks, ok_ref, local, *refs):
    priors, out_ref = refs[:-1], refs[-1]

    def write(j, out):
        write_partial(out_ref, heads, tokens, [(j, out)], None)

    lse = merged(heads, tokens, ok_ref, local, priors, checks, write)
    write_partial(out_ref, heads, tokens, [], lse)


def finish_kernel(heads, tokens, cols, parts, ok_ref, *refs):
    out_ref, stage, sems = refs[-3:]
    copies = []
    for first, checks in parts:
        local, priors, refs = refs[0], refs[1 : 1 + len(checks)], refs[1 + len(checks) :]

        def write(j, out):
            at = pl.ds((first + j) * tokens, tokens)
            stage[at, :] = out.T
            copy = pltpu.make_async_copy(
                stage.at[at].reshape(tokens // cols, cols, HDIM),
                out_ref.at[0, :, :, pl.ds((first + j) * HDIM, HDIM)],
                sems.at[first + j],
            )
            copy.start()
            copies.append(copy)

        merged(heads, tokens, ok_ref, local, priors, checks, write)
    for copy in copies:
        copy.wait()


def merge(heads, shape, ok, local, priors, checks):
    tokens = shape[0] * shape[1]
    return pl.pallas_call(
        functools.partial(merge_kernel, heads, tokens, checks),
        out_shape=partial_shape(heads, tokens),
        in_specs=[WHOLE] * (2 + len(priors)),
        out_specs=WHOLE,
        compiler_params=pltpu.CompilerParams(vmem_limit_bytes=8 * 2**20),
        cost_estimate=pl.CostEstimate(
            flops=10**8, bytes_accessed=8 * heads * tokens * HDIM, transcendentals=0
        ),
        name="merge",
    )(ok, local, *priors)


def finish(heads, shape, ok, *parts):
    rows, cols, channels = shape
    tokens = rows * cols
    args = [ok]
    for _, local, priors, _ in parts:
        args += [local, *priors]
    layout = tuple((first, checks) for first, _, _, checks in parts)
    return pl.pallas_call(
        functools.partial(finish_kernel, heads, tokens, cols, layout),
        out_shape=jax.ShapeDtypeStruct((1, rows, cols, channels), jnp.bfloat16),
        in_specs=[WHOLE] * len(args),
        out_specs=pl.BlockSpec(memory_space=pl.ANY),
        scratch_shapes=[
            pltpu.VMEM((tokens * channels // HDIM, HDIM), jnp.bfloat16),
            pltpu.SemaphoreType.DMA((channels // HDIM,)),
        ],
        compiler_params=pltpu.CompilerParams(vmem_limit_bytes=8 * 2**20),
        cost_estimate=pl.CostEstimate(
            flops=10**8, bytes_accessed=16 * heads * tokens * HDIM, transcendentals=0
        ),
        name="finish",
    )(*args)


def steps(queries, keys, values, window):
    _, rows, cols, channels = queries.shape
    args = (
        pltpu.with_memory_space_constraint(a, pltpu.HBM) for a in (queries, keys, values, window)
    )
    half = channels // HDIM // 2
    shape = (rows, cols, channels)
    go = functools.partial(attend, heads=half, shape=shape)
    qa, kva, qb, kvb, ok = pack(half, *args)

    a1 = shift(kva, "tm", 1)
    a2 = shift(a1, "tm", 1, skip=1)
    qm = shift(qa, "space", 1)
    qp = shift(qa, "space", -1)
    along = (kva, a1, a2)
    frames = [tuple(3 * back + dy for back in range(3)) for dy in range(3)]
    both, mine = (True, True), (False,)
    first, second, edge = ("tm", 0), ("tm", 1), ("space", 0)
    pair_cases = (
        ((first, edge), (1,), (0,)),
        ((first,), (0, 1), (0,)),
        ((second, edge), (1,), (0, 1)),
        ((second,), (0, 1), (0, 1)),
    )
    frame_cases = (((first,), (0,), (0,)), ((second,), (0,), (0, 1)))
    row_cases = (((edge,), (0,), (1, 2)), ((("space", -1),), (0,), (0, 1)))
    km, kp = go((frames[2], frames[0]), both, pair_cases, qs=(qm, qp), kvs=along)
    pp = shift(km, "space", -1)
    pm = shift(kp, "space", 1)
    (ka,) = go((frames[1],), mine, frame_cases, qs=(qa,), kvs=along)

    q1 = shift(qb, "tm", -1)
    q2 = shift(q1, "tm", -1, ahead=1)
    lo = shift(kvb, "space", 1)
    hi = shift(kvb, "space", -1)
    across = (lo, kvb, hi)
    offsets = [tuple(3 * back + dy for dy in range(3)) for back in range(3)]

    (k2,) = go((offsets[2],), (True,), row_cases, qs=(q2,), kvs=across)
    p2 = shift(k2, "tm", 1, ahead=1)
    (k1,) = go((offsets[1],), mine, row_cases, qs=(q1,), kvs=across)
    (k0,) = go((offsets[0],), mine, row_cases, qs=(qb,), kvs=across)
    m1 = merge(half, shape, ok, k1, (p2,), (FRAME_1,))
    p1 = shift(m1, "tm", 1)

    part_a = (0, ka, (pm, pp), (ROW_BEFORE, ROW_AFTER))
    part_b = (half, k0, (p1,), (FRAME_1,))
    return finish(half, shape, ok, part_a, part_b)


def solution(mesh):
    arrays = P(("group", "tm"), "space", None, "head")
    return jax.shard_map(
        steps,
        mesh=mesh,
        in_specs=(arrays, arrays, arrays, P(("group", "tm"), "space", None, None)),
        out_specs=arrays,
        check_vma=False,
    )
```

```python
import functools

import jax
import jax.numpy as jnp
from jax import lax
from jax.experimental import pallas as pl
from jax.experimental.pallas import tpu as pltpu
from jax.sharding import PartitionSpec as P


HDIM = 128
TILE = 8
SLOTS = 27
MASKS = 48
STATS = 8
NEVER = -1e30
FLOOR = -1e25
SCALE = (HDIM**-0.5) * 1.4426950408889634
WHOLE = pl.BlockSpec(memory_space=pltpu.VMEM)
ROW_BEFORE, ROW_AFTER, FRAME_1, FRAME_2 = range(4)
LAG = 6


def shift(block, axis, by, skip=0, ahead=0):
    size = lax.axis_size(axis)
    route = [
        (i, i + by)
        for i in range(skip, size)
        if 0 <= i + by < size and i + by + ahead < size and i + ahead < size
    ]
    return lax.ppermute(block, axis, route)


def masks(tcols, flags, window):
    row = lax.broadcasted_iota(jnp.int32, (MASKS, HDIM), 0)
    lane = lax.broadcasted_iota(jnp.int32, (MASKS, HDIM), 1)
    place, key_tile = lax.div(row, tcols), lax.rem(row, tcols)
    total = jnp.zeros((MASKS, HDIM), jnp.float32)
    for c in range(tcols):
        bits = jnp.broadcast_to(window[c : c + 1, :], (MASKS, SLOTS))
        bits = jnp.concatenate([bits, jnp.zeros((MASKS, HDIM - SLOTS), jnp.float32)], axis=1)
        step = key_tile - c
        bits = jnp.where((lane == place * 3 + step + 1) & (jnp.abs(step) <= 1), bits, 0.0)
        total = jnp.where(lane == c, jnp.sum(bits, axis=1, keepdims=True), total)
    own = (place == 1) & (key_tile == lane)
    back, dy = lax.div(place, 3), lax.rem(place, 3)
    ok = jnp.full((MASKS, HDIM), 1, jnp.int32)
    ok = jnp.where(dy == 0, flags[ROW_BEFORE], ok)
    ok = jnp.where(dy == 2, flags[ROW_AFTER], ok)
    ok = jnp.where(back == 1, ok * flags[FRAME_1], ok)
    ok = jnp.where(back == 2, ok * flags[FRAME_2], ok)
    allowed = ((total > 0.5) | own) & (ok > 0)
    return jnp.where(allowed | (lane >= tcols), 0.0, NEVER).astype(jnp.bfloat16)


def pack_kernel(heads, tokens, q_ref, k_ref, v_ref, w_ref, *refs):
    packed, ok_ref, (vbuf, wbuf, sems) = refs[:4], refs[4], refs[5:]
    table = pltpu.make_async_copy(w_ref.at[0, 0], wbuf, sems.at[6 * heads])
    table.start()
    rows, cols = q_ref.shape[1], q_ref.shape[2]
    copies = {}
    for n, src in enumerate((v_ref, k_ref, q_ref)):
        for head in range(2 * heads):
            half, j = divmod(head, heads)
            if n == 0:
                dst = vbuf.at[pl.ds(head * tokens, tokens)]
            else:
                dst = packed[2 * half + n % 2].at[pl.ds(j * tokens, tokens)]
            copy = pltpu.make_async_copy(
                src.at[0, :, :, pl.ds(head * HDIM, HDIM)],
                dst.reshape(rows, cols, HDIM),
                sems.at[3 * head + n],
            )
            copy.start()
            copies[n, head] = copy
    here, frame = lax.axis_index("space"), lax.axis_index("tm")
    tests = here > 0, here < lax.axis_size("space") - 1, frame > 0, frame > 1
    flags = [jnp.where(test, 1, 0) for test in tests]
    sub = lax.broadcasted_iota(jnp.int32, ok_ref.shape, 0)
    ok = jnp.zeros(ok_ref.shape, jnp.int32)
    for n, flag in enumerate(flags):
        ok = jnp.where(sub == n, flag, ok)
    ok_ref[...] = ok
    table.wait()
    mask = masks(cols // TILE, flags, wbuf[...].astype(jnp.float32))
    for half in range(2):
        packed[2 * half][heads * tokens :, :] = mask
    for head in range(2 * heads):
        copies[0, head].wait()
    for head in range(2 * heads):
        half, j = divmod(head, heads)
        vt = vbuf[head * tokens : (head + 1) * tokens, :].T
        for s in range(tokens // HDIM):
            at = (heads + j) * tokens + s * HDIM
            packed[2 * half + 1][at : at + HDIM, :] = vt[:, s * HDIM : (s + 1) * HDIM]
    for head in range(2 * heads):
        copies[1, head].wait()
        copies[2, head].wait()


def pack(heads, queries, keys, values, window):
    tokens = queries.shape[1] * queries.shape[2]
    shapes = [
        jax.ShapeDtypeStruct((heads * tokens + MASKS, HDIM), jnp.bfloat16),
        jax.ShapeDtypeStruct((2 * heads * tokens, HDIM), jnp.bfloat16),
    ]
    return pl.pallas_call(
        functools.partial(pack_kernel, heads, tokens),
        out_shape=shapes * 2 + [jax.ShapeDtypeStruct((STATS, HDIM), jnp.int32)],
        in_specs=[pl.BlockSpec(memory_space=pltpu.HBM)] * 4,
        out_specs=[WHOLE] * 5,
        scratch_shapes=[
            pltpu.VMEM((2 * heads * tokens, HDIM), jnp.bfloat16),
            pltpu.VMEM(window.shape[2:], window.dtype),
            pltpu.SemaphoreType.DMA((6 * heads + 1,)),
        ],
        compiler_params=pltpu.CompilerParams(vmem_limit_bytes=8 * 2**20),
        cost_estimate=pl.CostEstimate(
            flops=10**9, bytes_accessed=12 * heads * tokens * HDIM, transcendentals=0
        ),
        name="pack",
    )(queries, keys, values, window)


def side_by_side(ref, base, tokens):
    return jnp.concatenate(
        [ref[base + s * HDIM : base + (s + 1) * HDIM, :] for s in range(tokens // HDIM)], axis=1
    )


def write_partial(out_ref, heads, tokens, outs, lse):
    halves = tokens // HDIM
    for j, out in outs:
        for s in range(halves):
            at = j * tokens + s * HDIM
            out_ref[at : at + HDIM, :] = out[:, s * HDIM : (s + 1) * HDIM]
    if lse is not None:
        for p in range(3):
            part = lse.astype(jnp.bfloat16)
            lse = lse - part.astype(jnp.float32)
            for s in range(halves):
                at = heads * tokens + (p * halves + s) * STATS
                out_ref[at : at + STATS, :] = part[:, s * HDIM : (s + 1) * HDIM]


def read_lse(in_ref, heads, tokens):
    halves = tokens // HDIM
    parts = []
    for s in range(halves):
        part = jnp.zeros((STATS, HDIM), jnp.float32)
        for p in range(3):
            at = heads * tokens + (p * halves + s) * STATS
            part = part + in_ref[at : at + STATS, :].astype(jnp.float32)
        parts.append(part)
    return jnp.concatenate(parts, axis=1)


def attend_kernel(heads, tokens, cols, sets, packed, cases, *refs):
    q_refs, refs = refs[: len(sets)], refs[len(sets) :]
    blocks = len(sets[0])
    kvs, out_refs = refs[:blocks], refs[blocks:]
    run = functools.partial(attend_case, heads, tokens, cols, sets, packed, q_refs, kvs, out_refs)
    everything = tuple(range(len(sets))), tuple(range(blocks))
    rest = None
    for where, chosen, used in (*cases, ((), *everything)):
        hit = rest
        for axis, index in where:
            same = lax.axis_index(axis) == index % lax.axis_size(axis)
            hit = same if hit is None else hit & same
        if hit is None:
            run(chosen, used)
            return
        pl.when(hit)(functools.partial(run, chosen, used))
        rest = jnp.logical_not(hit) if rest is None else rest & jnp.logical_not(hit)


def attend_case(heads, tokens, cols, sets, packed, q_refs, kvs, out_refs, chosen, used):
    tcols = cols // TILE
    repeat = tokens // cols

    row = lax.broadcasted_iota(jnp.int32, (cols, HDIM), 0)
    lane = lax.broadcasted_iota(jnp.int32, (cols, HDIM), 1)
    tile = jnp.where(lane == lax.div(row, TILE), 1.0, 0.0).astype(jnp.bfloat16)
    tile = jnp.concatenate([tile] * repeat, axis=0)
    bias = {}
    for which in chosen:
        rows = q_refs[which][heads * tokens :, :].astype(jnp.float32)
        for n in used:
            at = sets[which][n] * tcols
            part = [
                jnp.broadcast_to(rows[at + c : at + c + 1, :], (TILE, HDIM)) for c in range(tcols)
            ]
            part = jnp.concatenate(part, axis=0).astype(jnp.bfloat16)
            bias[which, n] = jnp.concatenate([part] * repeat, axis=0)

    streams = [(which, j) for which in chosen for j in range(heads)]
    group = 3 if len(streams) % 3 == 0 else 1
    units = [
        (n, stream)
        for base in range(0, len(streams), group)
        for n in used
        for stream in streams[base : base + group]
    ]
    tops, totals, outs, ready = {}, {}, {}, {}
    sub = lax.broadcasted_iota(jnp.int32, (STATS, tokens), 0)
    lses = {which: jnp.full((STATS, tokens), NEVER, jnp.float32) for which in chosen}
    for i in range(len(units) + LAG):
        if i < len(units):
            n, key = units[i]
            which, j = key
            at = slice(j * tokens, (j + 1) * tokens)
            qcat = jnp.concatenate([q_refs[which][at, :], tile], axis=1)
            kcat = jnp.concatenate([kvs[n][at, :], bias[which, n]], axis=1)
            scores = lax.dot_general(
                kcat, qcat, (((1,), (1,)), ((), ())), preferred_element_type=jnp.float32
            )
            top = jnp.max(scores, axis=0, keepdims=True) * SCALE
            old = tops.get(key)
            top = jnp.maximum(top, FLOOR if old is None else old)
            tops[key] = top
            weights = jnp.exp2(scores * SCALE - top)
            total = jnp.sum(weights, axis=0, keepdims=True)
            fade = None if old is None else jnp.exp2(old - top)
            totals[key] = total if old is None else totals[key] * fade + total
            ready[i] = fade, weights.astype(jnp.bfloat16)
        if i >= LAG:
            n, key = units[i - LAG]
            which, j = key
            fade, weights = ready.pop(i - LAG)
            out = jnp.dot(
                side_by_side(kvs[n], (heads + j) * tokens, tokens),
                weights,
                preferred_element_type=jnp.float32,
            )
            outs[key] = out if fade is None else outs[key] * fade + out
            if n == used[-1]:
                total = totals[key]
                out = outs.pop(key) * (1.0 / jnp.maximum(total, 1e-30))
                lse = tops[key] + jnp.log2(total)
                lses[which] = jnp.where((sub == j) & (total > 0), lse, lses[which])
                if packed[which]:
                    write_partial(
                        out_refs[which], heads, tokens, [(j, out.astype(jnp.bfloat16))], None
                    )
                else:
                    out_refs[which][j * HDIM : (j + 1) * HDIM, :] = out
    for which, lse in lses.items():
        if packed[which]:
            write_partial(out_refs[which], heads, tokens, [], lse)
        else:
            out_refs[which][heads * HDIM :, :] = lse


def partial_shape(heads, tokens):
    stats = 3 * (tokens // HDIM) * STATS
    return jax.ShapeDtypeStruct((heads * tokens + stats, HDIM), jnp.bfloat16)


def attend(sets, packed, cases, heads, shape, qs, kvs):
    rows, cols, _ = shape
    tokens = rows * cols
    out_shape = [
        partial_shape(heads, tokens)
        if p
        else jax.ShapeDtypeStruct((heads * HDIM + STATS, tokens), jnp.float32)
        for p in packed
    ]
    return pl.pallas_call(
        functools.partial(attend_kernel, heads, tokens, cols, sets, packed, cases),
        out_shape=out_shape,
        in_specs=[WHOLE] * (len(qs) + len(kvs)),
        out_specs=[WHOLE] * len(packed),
        compiler_params=pltpu.CompilerParams(vmem_limit_bytes=16 * 2**20),
        cost_estimate=pl.CostEstimate(
            flops=10**9, bytes_accessed=8 * heads * tokens * HDIM, transcendentals=0
        ),
        name="attend",
    )(*qs, *kvs)


def merged(heads, tokens, ok_ref, local, priors, checks, write):
    lses = [local[heads * HDIM :, :]]
    for ref, flag in zip(priors, checks):
        ok = jnp.concatenate([ok_ref[flag : flag + 1, :]] * (tokens // HDIM), axis=1)
        lses.append(jnp.where(ok > 0, read_lse(ref, heads, tokens), NEVER))
    top = functools.reduce(jnp.maximum, lses)
    shares = [jnp.exp2(lse - top) for lse in lses]
    total = functools.reduce(jnp.add, shares)
    shares = [share * (1.0 / total) for share in shares]
    for j in range(heads):
        out = local[j * HDIM : (j + 1) * HDIM, :] * shares[0][j : j + 1, :]
        for ref, share in zip(priors, shares[1:]):
            piece = side_by_side(ref, j * tokens, tokens).astype(jnp.float32)
            out = out + piece * share[j : j + 1, :]
        write(j, out.astype(jnp.bfloat16))


def finish_kernel(heads, tokens, cols, parts, ok_ref, *refs):
    out_ref, stage, sems = refs[-3:]
    copies = []
    for first, checks in parts:
        local, priors, refs = refs[0], refs[1 : 1 + len(checks)], refs[1 + len(checks) :]

        def write(j, out):
            at = pl.ds((first + j) * tokens, tokens)
            stage[at, :] = out.T
            copy = pltpu.make_async_copy(
                stage.at[at].reshape(tokens // cols, cols, HDIM),
                out_ref.at[0, :, :, pl.ds((first + j) * HDIM, HDIM)],
                sems.at[first + j],
            )
            copy.start()
            copies.append(copy)

        merged(heads, tokens, ok_ref, local, priors, checks, write)
    for copy in copies:
        copy.wait()


def finish(heads, shape, ok, *parts):
    rows, cols, channels = shape
    tokens = rows * cols
    args = [ok]
    for _, local, priors, _ in parts:
        args += [local, *priors]
    layout = tuple((first, checks) for first, _, _, checks in parts)
    return pl.pallas_call(
        functools.partial(finish_kernel, heads, tokens, cols, layout),
        out_shape=jax.ShapeDtypeStruct((1, rows, cols, channels), jnp.bfloat16),
        in_specs=[WHOLE] * len(args),
        out_specs=pl.BlockSpec(memory_space=pl.ANY),
        scratch_shapes=[
            pltpu.VMEM((tokens * channels // HDIM, HDIM), jnp.bfloat16),
            pltpu.SemaphoreType.DMA((channels // HDIM,)),
        ],
        compiler_params=pltpu.CompilerParams(vmem_limit_bytes=8 * 2**20),
        cost_estimate=pl.CostEstimate(
            flops=10**8, bytes_accessed=16 * heads * tokens * HDIM, transcendentals=0
        ),
        name="finish",
    )(*args)


def steps(queries, keys, values, window):
    _, rows, cols, channels = queries.shape
    args = (
        pltpu.with_memory_space_constraint(a, pltpu.HBM) for a in (queries, keys, values, window)
    )
    half = channels // HDIM // 2
    shape = (rows, cols, channels)
    go = functools.partial(attend, heads=half, shape=shape)
    qa, kva, qb, kvb, ok = pack(half, *args)

    a1 = shift(kva, "tm", 1)
    a2 = shift(a1, "tm", 1, skip=1)
    qm = shift(qa, "space", 1)
    qp = shift(qa, "space", -1)
    along = (kva, a1, a2)
    frames = [tuple(3 * back + dy for back in range(3)) for dy in range(3)]
    both, mine = (True, True), (False,)
    first, second, edge = ("tm", 0), ("tm", 1), ("space", 0)
    pair_cases = (
        ((first, edge), (1,), (0,)),
        ((first,), (0, 1), (0,)),
        ((second, edge), (1,), (0, 1)),
        ((second,), (0, 1), (0, 1)),
    )
    frame_cases = (((first,), (0,), (0,)), ((second,), (0,), (0, 1)))
    row_cases = (((edge,), (0,), (1, 2)), ((("space", -1),), (0,), (0, 1)))
    km, kp = go((frames[2], frames[0]), both, pair_cases, qs=(qm, qp), kvs=along)
    pp = shift(km, "space", -1)
    pm = shift(kp, "space", 1)
    (ka,) = go((frames[1],), mine, frame_cases, qs=(qa,), kvs=along)

    q1 = shift(qb, "tm", -1)
    q2 = shift(q1, "tm", -1, ahead=1)
    lo = shift(kvb, "space", 1)
    hi = shift(kvb, "space", -1)
    across = (lo, kvb, hi)
    offsets = [tuple(3 * back + dy for dy in range(3)) for back in range(3)]

    (k2,) = go((offsets[2],), (True,), row_cases, qs=(q2,), kvs=across)
    p2 = shift(k2, "tm", 2)
    (k1,) = go((offsets[1],), (True,), row_cases, qs=(q1,), kvs=across)
    p1 = shift(k1, "tm", 1)
    (k0,) = go((offsets[0],), mine, row_cases, qs=(qb,), kvs=across)

    part_a = (0, ka, (pm, pp), (ROW_BEFORE, ROW_AFTER))
    part_b = (half, k0, (p1, p2), (FRAME_1, FRAME_2))
    return finish(half, shape, ok, part_a, part_b)


def solution(mesh):
    arrays = P(("group", "tm"), "space", None, "head")
    return jax.shard_map(
        steps,
        mesh=mesh,
        in_specs=(arrays, arrays, arrays, P(("group", "tm"), "space", None, None)),
        out_specs=arrays,
        check_vma=False,
    )
```

```python
import functools
import itertools

import jax
import jax.numpy as jnp
from jax import lax
from jax.experimental import pallas as pl
from jax.experimental.pallas import tpu as pltpu
from jax.sharding import PartitionSpec as P


HDIM = 128
TILE = 8
SLOTS = 27
MASKS = 48
STATS = 8
NEVER = -1e30
FLOOR = -1e25
SCALE = (HDIM**-0.5) * 1.4426950408889634
WHOLE = pl.BlockSpec(memory_space=pltpu.VMEM)
ROW_BEFORE, ROW_AFTER, FRAME_1, FRAME_2 = range(4)
LAG = 6


def shift(block, axis, by, skip=0, ahead=0):
    size = lax.axis_size(axis)
    route = [
        (i, i + by)
        for i in range(skip, size)
        if 0 <= i + by < size and i + by + ahead < size and i + ahead < size
    ]
    return lax.ppermute(block, axis, route)


def hop(block, axes, by, pick):
    sizes = [lax.axis_size(axis) for axis in axes]
    route = []
    for place in itertools.product(*map(range, sizes)):
        to = [p + b for p, b in zip(place, by)]
        if pick(place) and all(0 <= t < n for t, n in zip(to, sizes)):
            route.append((place[0] * sizes[1] + place[1], to[0] * sizes[1] + to[1]))
    return lax.ppermute(block, axes, route)


def masks(tcols, flags, window):
    row = lax.broadcasted_iota(jnp.int32, (MASKS, HDIM), 0)
    lane = lax.broadcasted_iota(jnp.int32, (MASKS, HDIM), 1)
    place, key_tile = lax.div(row, tcols), lax.rem(row, tcols)
    total = jnp.zeros((MASKS, HDIM), jnp.float32)
    for c in range(tcols):
        bits = jnp.broadcast_to(window[c : c + 1, :], (MASKS, SLOTS))
        bits = jnp.concatenate([bits, jnp.zeros((MASKS, HDIM - SLOTS), jnp.float32)], axis=1)
        step = key_tile - c
        bits = jnp.where((lane == place * 3 + step + 1) & (jnp.abs(step) <= 1), bits, 0.0)
        total = jnp.where(lane == c, jnp.sum(bits, axis=1, keepdims=True), total)
    own = (place == 1) & (key_tile == lane)
    back, dy = lax.div(place, 3), lax.rem(place, 3)
    ok = jnp.full((MASKS, HDIM), 1, jnp.int32)
    ok = jnp.where(dy == 0, flags[ROW_BEFORE], ok)
    ok = jnp.where(dy == 2, flags[ROW_AFTER], ok)
    ok = jnp.where(back == 1, ok * flags[FRAME_1], ok)
    ok = jnp.where(back == 2, ok * flags[FRAME_2], ok)
    allowed = ((total > 0.5) | own) & (ok > 0)
    return jnp.where(allowed | (lane >= tcols), 0.0, NEVER).astype(jnp.bfloat16)


def pack_kernel(heads, tokens, q_ref, k_ref, v_ref, w_ref, *refs):
    packed, ok_ref, (vbuf, wbuf, sems) = refs[:4], refs[4], refs[5:]
    table = pltpu.make_async_copy(w_ref.at[0, 0], wbuf, sems.at[6 * heads])
    table.start()
    rows, cols = q_ref.shape[1], q_ref.shape[2]
    copies = {}
    for n, src in enumerate((v_ref, k_ref, q_ref)):
        for head in range(2 * heads):
            half, j = divmod(head, heads)
            if n == 0:
                dst = vbuf.at[pl.ds(head * tokens, tokens)]
            else:
                dst = packed[2 * half + n % 2].at[pl.ds(j * tokens, tokens)]
            copy = pltpu.make_async_copy(
                src.at[0, :, :, pl.ds(head * HDIM, HDIM)],
                dst.reshape(rows, cols, HDIM),
                sems.at[3 * head + n],
            )
            copy.start()
            copies[n, head] = copy
    here, frame = lax.axis_index("space"), lax.axis_index("tm")
    tests = here > 0, here < lax.axis_size("space") - 1, frame > 0, frame > 1
    flags = [jnp.where(test, 1, 0) for test in tests]
    sub = lax.broadcasted_iota(jnp.int32, ok_ref.shape, 0)
    ok = jnp.zeros(ok_ref.shape, jnp.int32)
    for n, flag in enumerate(flags):
        ok = jnp.where(sub == n, flag, ok)
    ok_ref[...] = ok
    table.wait()
    mask = masks(cols // TILE, flags, wbuf[...].astype(jnp.float32))
    for half in range(2):
        packed[2 * half][heads * tokens :, :] = mask
    for head in range(2 * heads):
        copies[0, head].wait()
    for head in range(2 * heads):
        half, j = divmod(head, heads)
        vt = vbuf[head * tokens : (head + 1) * tokens, :].T
        for s in range(tokens // HDIM):
            at = (heads + j) * tokens + s * HDIM
            packed[2 * half + 1][at : at + HDIM, :] = vt[:, s * HDIM : (s + 1) * HDIM]
    for head in range(2 * heads):
        copies[1, head].wait()
        copies[2, head].wait()


def pack(heads, queries, keys, values, window):
    tokens = queries.shape[1] * queries.shape[2]
    shapes = [
        jax.ShapeDtypeStruct((heads * tokens + MASKS, HDIM), jnp.bfloat16),
        jax.ShapeDtypeStruct((2 * heads * tokens, HDIM), jnp.bfloat16),
    ]
    return pl.pallas_call(
        functools.partial(pack_kernel, heads, tokens),
        out_shape=shapes * 2 + [jax.ShapeDtypeStruct((STATS, HDIM), jnp.int32)],
        in_specs=[pl.BlockSpec(memory_space=pltpu.HBM)] * 4,
        out_specs=[WHOLE] * 5,
        scratch_shapes=[
            pltpu.VMEM((2 * heads * tokens, HDIM), jnp.bfloat16),
            pltpu.VMEM(window.shape[2:], window.dtype),
            pltpu.SemaphoreType.DMA((6 * heads + 1,)),
        ],
        compiler_params=pltpu.CompilerParams(vmem_limit_bytes=8 * 2**20),
        cost_estimate=pl.CostEstimate(
            flops=10**9, bytes_accessed=12 * heads * tokens * HDIM, transcendentals=0
        ),
        name="pack",
    )(queries, keys, values, window)


def side_by_side(ref, base, tokens):
    return jnp.concatenate(
        [ref[base + s * HDIM : base + (s + 1) * HDIM, :] for s in range(tokens // HDIM)], axis=1
    )


def write_partial(out_ref, heads, tokens, outs, lse):
    halves = tokens // HDIM
    for j, out in outs:
        for s in range(halves):
            at = j * tokens + s * HDIM
            out_ref[at : at + HDIM, :] = out[:, s * HDIM : (s + 1) * HDIM]
    if lse is not None:
        for p in range(3):
            part = lse.astype(jnp.bfloat16)
            lse = lse - part.astype(jnp.float32)
            for s in range(halves):
                at = heads * tokens + (p * halves + s) * STATS
                out_ref[at : at + STATS, :] = part[:, s * HDIM : (s + 1) * HDIM]


def read_lse(in_ref, heads, tokens):
    halves = tokens // HDIM
    parts = []
    for s in range(halves):
        part = jnp.zeros((STATS, HDIM), jnp.float32)
        for p in range(3):
            at = heads * tokens + (p * halves + s) * STATS
            part = part + in_ref[at : at + STATS, :].astype(jnp.float32)
        parts.append(part)
    return jnp.concatenate(parts, axis=1)


def attend_kernel(heads, tokens, cols, sets, packed, cases, *refs):
    q_refs, refs = refs[: len(sets)], refs[len(sets) :]
    blocks = len(sets[0])
    kvs, out_refs = refs[:blocks], refs[blocks:]
    run = functools.partial(attend_case, heads, tokens, cols, sets, packed, q_refs, kvs, out_refs)
    everything = tuple(range(len(sets))), tuple(range(blocks))
    rest = None
    for where, chosen, used in (*cases, ((), *everything)):
        hit = rest
        for axis, index in where:
            same = lax.axis_index(axis) == index % lax.axis_size(axis)
            hit = same if hit is None else hit & same
        if hit is None:
            run(chosen, used)
            return
        pl.when(hit)(functools.partial(run, chosen, used))
        if not where:
            return
        rest = jnp.logical_not(hit) if rest is None else rest & jnp.logical_not(hit)


def attend_case(heads, tokens, cols, sets, packed, q_refs, kvs, out_refs, chosen, used):
    tcols = cols // TILE
    repeat = tokens // cols

    row = lax.broadcasted_iota(jnp.int32, (cols, HDIM), 0)
    lane = lax.broadcasted_iota(jnp.int32, (cols, HDIM), 1)
    tile = jnp.where(lane == lax.div(row, TILE), 1.0, 0.0).astype(jnp.bfloat16)
    tile = jnp.concatenate([tile] * repeat, axis=0)
    bias = {}
    for which in chosen:
        rows = q_refs[which][heads * tokens :, :].astype(jnp.float32)
        for n in used:
            at = sets[which][n] * tcols
            part = [
                jnp.broadcast_to(rows[at + c : at + c + 1, :], (TILE, HDIM)) for c in range(tcols)
            ]
            part = jnp.concatenate(part, axis=0).astype(jnp.bfloat16)
            bias[which, n] = jnp.concatenate([part] * repeat, axis=0)

    streams = [(which, j) for which in chosen for j in range(heads)]
    group = 3 if len(streams) % 3 == 0 else 1
    units = [
        (n, stream)
        for base in range(0, len(streams), group)
        for n in used
        for stream in streams[base : base + group]
    ]
    tops, totals, outs, ready = {}, {}, {}, {}
    sub = lax.broadcasted_iota(jnp.int32, (STATS, tokens), 0)
    lses = {which: jnp.full((STATS, tokens), NEVER, jnp.float32) for which in chosen}
    for i in range(len(units) + LAG):
        if i < len(units):
            n, key = units[i]
            which, j = key
            at = slice(j * tokens, (j + 1) * tokens)
            qcat = jnp.concatenate([q_refs[which][at, :], tile], axis=1)
            kcat = jnp.concatenate([kvs[n][at, :], bias[which, n]], axis=1)
            scores = lax.dot_general(
                kcat, qcat, (((1,), (1,)), ((), ())), preferred_element_type=jnp.float32
            )
            top = jnp.max(scores, axis=0, keepdims=True) * SCALE
            old = tops.get(key)
            top = jnp.maximum(top, FLOOR if old is None else old)
            tops[key] = top
            weights = jnp.exp2(scores * SCALE - top)
            total = jnp.sum(weights, axis=0, keepdims=True)
            fade = None if old is None else jnp.exp2(old - top)
            totals[key] = total if old is None else totals[key] * fade + total
            ready[i] = fade, weights.astype(jnp.bfloat16)
        if i >= LAG:
            n, key = units[i - LAG]
            which, j = key
            fade, weights = ready.pop(i - LAG)
            out = jnp.dot(
                side_by_side(kvs[n], (heads + j) * tokens, tokens),
                weights,
                preferred_element_type=jnp.float32,
            )
            outs[key] = out if fade is None else outs[key] * fade + out
            if n == used[-1]:
                total = totals[key]
                out = outs.pop(key) * (1.0 / jnp.maximum(total, 1e-30))
                lse = tops[key] + jnp.log2(total)
                lses[which] = jnp.where((sub == j) & (total > 0), lse, lses[which])
                if packed[which % len(packed)]:
                    piece = [(j, out.astype(jnp.bfloat16))]
                    write_partial(out_refs[which % len(out_refs)], heads, tokens, piece, None)
                else:
                    out_refs[which % len(out_refs)][j * HDIM : (j + 1) * HDIM, :] = out
    for which, lse in lses.items():
        if packed[which % len(packed)]:
            write_partial(out_refs[which % len(out_refs)], heads, tokens, [], lse)
        else:
            out_refs[which % len(out_refs)][heads * HDIM :, :] = lse


def partial_shape(heads, tokens):
    stats = 3 * (tokens // HDIM) * STATS
    return jax.ShapeDtypeStruct((heads * tokens + stats, HDIM), jnp.bfloat16)


def attend(sets, packed, cases, heads, shape, qs, kvs):
    rows, cols, _ = shape
    tokens = rows * cols
    out_shape = [
        partial_shape(heads, tokens)
        if p
        else jax.ShapeDtypeStruct((heads * HDIM + STATS, tokens), jnp.float32)
        for p in packed
    ]
    return pl.pallas_call(
        functools.partial(attend_kernel, heads, tokens, cols, sets, packed, cases),
        out_shape=out_shape,
        in_specs=[WHOLE] * (len(qs) + len(kvs)),
        out_specs=[WHOLE] * len(packed),
        compiler_params=pltpu.CompilerParams(vmem_limit_bytes=16 * 2**20),
        cost_estimate=pl.CostEstimate(
            flops=10**9, bytes_accessed=8 * heads * tokens * HDIM, transcendentals=0
        ),
        name="attend",
    )(*qs, *kvs)


def merged(heads, tokens, ok_ref, local, priors, checks, write):
    lses = [local[heads * HDIM :, :]]
    for ref, flag in zip(priors, checks):
        ok = jnp.concatenate([ok_ref[flag : flag + 1, :]] * (tokens // HDIM), axis=1)
        lses.append(jnp.where(ok > 0, read_lse(ref, heads, tokens), NEVER))
    top = functools.reduce(jnp.maximum, lses)
    shares = [jnp.exp2(lse - top) for lse in lses]
    total = functools.reduce(jnp.add, shares)
    shares = [share * (1.0 / total) for share in shares]
    for j in range(heads):
        out = local[j * HDIM : (j + 1) * HDIM, :] * shares[0][j : j + 1, :]
        for ref, share in zip(priors, shares[1:]):
            piece = side_by_side(ref, j * tokens, tokens).astype(jnp.float32)
            out = out + piece * share[j : j + 1, :]
        write(j, out.astype(jnp.bfloat16))


def finish_kernel(heads, tokens, cols, first, checks, ok_ref, local, *refs):
    priors = refs[: len(checks)]
    out_ref, stage, sems = refs[-3:]
    copies = []

    def write(j, out):
        at = pl.ds(j * tokens, tokens)
        stage[at, :] = out.T
        copy = pltpu.make_async_copy(
            stage.at[at].reshape(tokens // cols, cols, HDIM),
            out_ref.at[0, :, :, pl.ds((first + j) * HDIM, HDIM)],
            sems.at[j],
        )
        copy.start()
        copies.append(copy)

    merged(heads, tokens, ok_ref, local, priors, checks, write)
    for copy in copies:
        copy.wait()


def finish(heads, shape, ok, first, local, priors, checks, into=None):
    rows, cols, channels = shape
    tokens = rows * cols
    args, aliases = [ok, local, *priors], {}
    specs = [WHOLE] * len(args)
    if into is not None:
        aliases = {len(args): 0}
        args.append(into)
        specs.append(pl.BlockSpec(memory_space=pl.ANY))
    return pl.pallas_call(
        functools.partial(finish_kernel, heads, tokens, cols, first, checks),
        out_shape=jax.ShapeDtypeStruct((1, rows, cols, channels), jnp.bfloat16),
        in_specs=specs,
        out_specs=pl.BlockSpec(memory_space=pl.ANY),
        input_output_aliases=aliases,
        scratch_shapes=[
            pltpu.VMEM((heads * tokens, HDIM), jnp.bfloat16),
            pltpu.SemaphoreType.DMA((heads,)),
        ],
        compiler_params=pltpu.CompilerParams(vmem_limit_bytes=8 * 2**20),
        cost_estimate=pl.CostEstimate(
            flops=10**8, bytes_accessed=8 * heads * tokens * HDIM, transcendentals=0
        ),
        name="finish",
    )(*args)


def steps(queries, keys, values, window):
    _, rows, cols, channels = queries.shape
    args = (
        pltpu.with_memory_space_constraint(a, pltpu.HBM) for a in (queries, keys, values, window)
    )
    half = channels // HDIM // 2
    shape = (rows, cols, channels)
    go = functools.partial(attend, heads=half, shape=shape)
    qa, kva, qb, kvb, ok = pack(half, *args)

    a1 = shift(kva, "tm", 1)
    a2 = shift(a1, "tm", 1, skip=1)
    qm = shift(qa, "space", 1)
    qp = shift(qa, "space", -1)
    along = (kva, a1, a2)
    frames = [tuple(3 * back + dy for back in range(3)) for dy in range(3)]
    both, mine = (True, True), (False,)
    first, second, edge = ("tm", 0), ("tm", 1), ("space", 0)
    pair_cases = (
        ((first, edge), (1,), (0,)),
        ((first,), (0, 1), (0,)),
        ((second, edge), (1,), (0, 1)),
        ((second,), (0, 1), (0, 1)),
    )
    frame_cases = (((first,), (0,), (0,)), ((second,), (0,), (0, 1)))
    km, kp = go((frames[2], frames[0]), both, pair_cases, qs=(qm, qp), kvs=along)
    pp = shift(km, "space", -1)
    pm = shift(kp, "space", 1)
    (ka,) = go((frames[1],), mine, frame_cases, qs=(qa,), kvs=along)

    grid = ("tm", "space")
    below, beside = (1, 0), (0, 1)
    q1 = hop(qb, grid, (-1, 0), lambda place: place != below)
    q1_late = hop(qb, grid, (-1, 0), lambda place: place == below)
    hi = hop(kvb, grid, (0, -1), lambda place: place != beside)
    hi_late = hop(kvb, grid, (0, -1), lambda place: place == beside)
    q2 = shift(q1, "tm", -1, ahead=1)
    lo = shift(kvb, "space", 1)
    across = (lo, kvb, hi, hi_late)
    offsets = [tuple(3 * back + dy for dy in (0, 1, 2, 2)) for back in range(3)]

    def row_cases(late=0):
        return (
            ((first, edge), (late,), (1, 3)),
            ((edge,), (0,), (1, 2)),
            ((("space", -1),), (0,), (0, 1)),
            ((), (0,), (0, 1, 2)),
        )

    (k2,) = go((offsets[2],), (True,), row_cases(), qs=(q2,), kvs=across)
    p2 = shift(k2, "tm", 2)
    (k1,) = go((offsets[1],) * 2, (True,), row_cases(1), qs=(q1, q1_late), kvs=across)
    p1 = shift(k1, "tm", 1)
    (k0,) = go((offsets[0],), mine, row_cases(), qs=(qb,), kvs=across)

    out = finish(half, shape, ok, half, k0, (p1, p2), (FRAME_1, FRAME_2))
    return finish(half, shape, ok, 0, ka, (pm, pp), (ROW_BEFORE, ROW_AFTER), into=out)


def solution(mesh):
    arrays = P(("group", "tm"), "space", None, "head")
    return jax.shard_map(
        steps,
        mesh=mesh,
        in_specs=(arrays, arrays, arrays, P(("group", "tm"), "space", None, None)),
        out_specs=arrays,
        check_vma=False,
    )
```

```python
import functools
import itertools

import jax
import jax.numpy as jnp
from jax import lax
from jax.experimental import pallas as pl
from jax.experimental.pallas import tpu as pltpu
from jax.sharding import PartitionSpec as P


HDIM = 128
TILE = 8
SLOTS = 27
MASKS = 48
STATS = 8
NEVER = -1e30
FLOOR = -1e25
SCALE = (HDIM**-0.5) * 1.4426950408889634
WHOLE = pl.BlockSpec(memory_space=pltpu.VMEM)
ROW_BEFORE, ROW_AFTER, FRAME_1, FRAME_2 = range(4)
LAG = 6


def shift(block, axis, by, skip=0, ahead=0):
    size = lax.axis_size(axis)
    route = [
        (i, i + by)
        for i in range(skip, size)
        if 0 <= i + by < size and i + by + ahead < size and i + ahead < size
    ]
    return lax.ppermute(block, axis, route)


def hop(block, axes, by, pick):
    sizes = [lax.axis_size(axis) for axis in axes]
    route = []
    for place in itertools.product(*map(range, sizes)):
        to = [p + b for p, b in zip(place, by)]
        if pick(place) and all(0 <= t < n for t, n in zip(to, sizes)):
            route.append((place[0] * sizes[1] + place[1], to[0] * sizes[1] + to[1]))
    return lax.ppermute(block, axes, route)


def masks(tcols, flags, window):
    row = lax.broadcasted_iota(jnp.int32, (MASKS, HDIM), 0)
    lane = lax.broadcasted_iota(jnp.int32, (MASKS, HDIM), 1)
    place, key_tile = lax.div(row, tcols), lax.rem(row, tcols)
    total = jnp.zeros((MASKS, HDIM), jnp.float32)
    for c in range(tcols):
        bits = jnp.broadcast_to(window[c : c + 1, :], (MASKS, SLOTS))
        bits = jnp.concatenate([bits, jnp.zeros((MASKS, HDIM - SLOTS), jnp.float32)], axis=1)
        step = key_tile - c
        bits = jnp.where((lane == place * 3 + step + 1) & (jnp.abs(step) <= 1), bits, 0.0)
        total = jnp.where(lane == c, jnp.sum(bits, axis=1, keepdims=True), total)
    own = (place == 1) & (key_tile == lane)
    back, dy = lax.div(place, 3), lax.rem(place, 3)
    ok = jnp.full((MASKS, HDIM), 1, jnp.int32)
    ok = jnp.where(dy == 0, flags[ROW_BEFORE], ok)
    ok = jnp.where(dy == 2, flags[ROW_AFTER], ok)
    ok = jnp.where(back == 1, ok * flags[FRAME_1], ok)
    ok = jnp.where(back == 2, ok * flags[FRAME_2], ok)
    allowed = ((total > 0.5) | own) & (ok > 0)
    return jnp.where(allowed | (lane >= tcols), 0.0, NEVER).astype(jnp.bfloat16)


def pack_kernel(heads, tokens, q_ref, k_ref, v_ref, w_ref, *refs):
    packed, ok_ref, (vbuf, wbuf, sems) = refs[:4], refs[4], refs[5:]
    table = pltpu.make_async_copy(w_ref.at[0, 0], wbuf, sems.at[6 * heads])
    table.start()
    rows, cols = q_ref.shape[1], q_ref.shape[2]
    copies = {}
    for n, src in enumerate((v_ref, k_ref, q_ref)):
        for head in range(2 * heads):
            half, j = divmod(head, heads)
            if n == 0:
                dst = vbuf.at[pl.ds(head * tokens, tokens)]
            else:
                dst = packed[2 * half + n % 2].at[pl.ds(j * tokens, tokens)]
            copy = pltpu.make_async_copy(
                src.at[0, :, :, pl.ds(head * HDIM, HDIM)],
                dst.reshape(rows, cols, HDIM),
                sems.at[3 * head + n],
            )
            copy.start()
            copies[n, head] = copy
    here, frame = lax.axis_index("space"), lax.axis_index("tm")
    tests = here > 0, here < lax.axis_size("space") - 1, frame > 0, frame > 1
    flags = [jnp.where(test, 1, 0) for test in tests]
    sub = lax.broadcasted_iota(jnp.int32, ok_ref.shape, 0)
    ok = jnp.zeros(ok_ref.shape, jnp.int32)
    for n, flag in enumerate(flags):
        ok = jnp.where(sub == n, flag, ok)
    ok_ref[...] = ok
    table.wait()
    mask = masks(cols // TILE, flags, wbuf[...].astype(jnp.float32))
    for half in range(2):
        packed[2 * half][heads * tokens :, :] = mask
    for head in range(2 * heads):
        copies[0, head].wait()
    for head in range(2 * heads):
        half, j = divmod(head, heads)
        vt = vbuf[head * tokens : (head + 1) * tokens, :].T
        for s in range(tokens // HDIM):
            at = (heads + j) * tokens + s * HDIM
            packed[2 * half + 1][at : at + HDIM, :] = vt[:, s * HDIM : (s + 1) * HDIM]
    for head in range(2 * heads):
        copies[1, head].wait()
        copies[2, head].wait()


def pack(heads, queries, keys, values, window):
    tokens = queries.shape[1] * queries.shape[2]
    shapes = [
        jax.ShapeDtypeStruct((heads * tokens + MASKS, HDIM), jnp.bfloat16),
        jax.ShapeDtypeStruct((2 * heads * tokens, HDIM), jnp.bfloat16),
    ]
    return pl.pallas_call(
        functools.partial(pack_kernel, heads, tokens),
        out_shape=shapes * 2 + [jax.ShapeDtypeStruct((STATS, HDIM), jnp.int32)],
        in_specs=[pl.BlockSpec(memory_space=pltpu.HBM)] * 4,
        out_specs=[WHOLE] * 5,
        scratch_shapes=[
            pltpu.VMEM((2 * heads * tokens, HDIM), jnp.bfloat16),
            pltpu.VMEM(window.shape[2:], window.dtype),
            pltpu.SemaphoreType.DMA((6 * heads + 1,)),
        ],
        compiler_params=pltpu.CompilerParams(vmem_limit_bytes=8 * 2**20),
        cost_estimate=pl.CostEstimate(
            flops=10**9, bytes_accessed=12 * heads * tokens * HDIM, transcendentals=0
        ),
        name="pack",
    )(queries, keys, values, window)


def side_by_side(ref, base, tokens):
    return jnp.concatenate(
        [ref[base + s * HDIM : base + (s + 1) * HDIM, :] for s in range(tokens // HDIM)], axis=1
    )


def write_partial(out_ref, heads, tokens, outs, lse):
    halves = tokens // HDIM
    for j, out in outs:
        for s in range(halves):
            at = j * tokens + s * HDIM
            out_ref[at : at + HDIM, :] = out[:, s * HDIM : (s + 1) * HDIM]
    if lse is not None:
        for p in range(3):
            part = lse.astype(jnp.bfloat16)
            lse = lse - part.astype(jnp.float32)
            for s in range(halves):
                at = heads * tokens + (p * halves + s) * STATS
                out_ref[at : at + STATS, :] = part[:, s * HDIM : (s + 1) * HDIM]


def read_lse(in_ref, heads, tokens):
    halves = tokens // HDIM
    parts = []
    for s in range(halves):
        part = jnp.zeros((STATS, HDIM), jnp.float32)
        for p in range(3):
            at = heads * tokens + (p * halves + s) * STATS
            part = part + in_ref[at : at + STATS, :].astype(jnp.float32)
        parts.append(part)
    return jnp.concatenate(parts, axis=1)


def attend_kernel(heads, tokens, cols, sets, packed, cases, *refs):
    q_refs, refs = refs[: len(sets)], refs[len(sets) :]
    blocks = len(sets[0])
    kvs, out_refs = refs[:blocks], refs[blocks:]
    run = functools.partial(attend_case, heads, tokens, cols, sets, packed, q_refs, kvs, out_refs)
    everything = tuple(range(len(sets))), tuple(range(blocks))
    rest = None
    for where, chosen, used in (*cases, ((), *everything)):
        hit = rest
        for axis, index in where:
            same = lax.axis_index(axis) == index % lax.axis_size(axis)
            hit = same if hit is None else hit & same
        if hit is None:
            run(chosen, used)
            return
        pl.when(hit)(functools.partial(run, chosen, used))
        if not where:
            return
        rest = jnp.logical_not(hit) if rest is None else rest & jnp.logical_not(hit)


def attend_case(heads, tokens, cols, sets, packed, q_refs, kvs, out_refs, chosen, used):
    tcols = cols // TILE
    repeat = tokens // cols

    row = lax.broadcasted_iota(jnp.int32, (cols, HDIM), 0)
    lane = lax.broadcasted_iota(jnp.int32, (cols, HDIM), 1)
    tile = jnp.where(lane == lax.div(row, TILE), 1.0, 0.0).astype(jnp.bfloat16)
    tile = jnp.concatenate([tile] * repeat, axis=0)
    bias = {}
    for which in chosen:
        rows = q_refs[which][heads * tokens :, :].astype(jnp.float32)
        for n in used:
            at = sets[which][n] * tcols
            part = [
                jnp.broadcast_to(rows[at + c : at + c + 1, :], (TILE, HDIM)) for c in range(tcols)
            ]
            part = jnp.concatenate(part, axis=0).astype(jnp.bfloat16)
            bias[which, n] = jnp.concatenate([part] * repeat, axis=0)

    streams = [(which, j) for which in chosen for j in range(heads)]
    group = 3 if len(streams) % 3 == 0 else 1
    units = [
        (n, stream)
        for base in range(0, len(streams), group)
        for n in used
        for stream in streams[base : base + group]
    ]
    tops, totals, outs, ready = {}, {}, {}, {}
    sub = lax.broadcasted_iota(jnp.int32, (STATS, tokens), 0)
    lses = {which: jnp.full((STATS, tokens), NEVER, jnp.float32) for which in chosen}
    for i in range(len(units) + LAG):
        if i < len(units):
            n, key = units[i]
            which, j = key
            at = slice(j * tokens, (j + 1) * tokens)
            qcat = jnp.concatenate([q_refs[which][at, :], tile], axis=1)
            kcat = jnp.concatenate([kvs[n][at, :], bias[which, n]], axis=1)
            scores = lax.dot_general(
                kcat, qcat, (((1,), (1,)), ((), ())), preferred_element_type=jnp.float32
            )
            top = jnp.max(scores, axis=0, keepdims=True) * SCALE
            old = tops.get(key)
            top = jnp.maximum(top, FLOOR if old is None else old)
            tops[key] = top
            weights = jnp.exp2(scores * SCALE - top)
            total = jnp.sum(weights, axis=0, keepdims=True)
            fade = None if old is None else jnp.exp2(old - top)
            totals[key] = total if old is None else totals[key] * fade + total
            ready[i] = fade, weights.astype(jnp.bfloat16)
        if i >= LAG:
            n, key = units[i - LAG]
            which, j = key
            fade, weights = ready.pop(i - LAG)
            out = jnp.dot(
                side_by_side(kvs[n], (heads + j) * tokens, tokens),
                weights,
                preferred_element_type=jnp.float32,
            )
            outs[key] = out if fade is None else outs[key] * fade + out
            if n == used[-1]:
                total = totals[key]
                out = outs.pop(key) * (1.0 / jnp.maximum(total, 1e-30))
                lse = tops[key] + jnp.log2(total)
                lses[which] = jnp.where((sub == j) & (total > 0), lse, lses[which])
                if packed[which % len(packed)]:
                    piece = [(j, out.astype(jnp.bfloat16))]
                    write_partial(out_refs[which % len(out_refs)], heads, tokens, piece, None)
                else:
                    out_refs[which % len(out_refs)][j * HDIM : (j + 1) * HDIM, :] = out
    for which, lse in lses.items():
        if packed[which % len(packed)]:
            write_partial(out_refs[which % len(out_refs)], heads, tokens, [], lse)
        else:
            out_refs[which % len(out_refs)][heads * HDIM :, :] = lse


def partial_shape(heads, tokens):
    stats = 3 * (tokens // HDIM) * STATS
    return jax.ShapeDtypeStruct((heads * tokens + stats, HDIM), jnp.bfloat16)


def attend(sets, packed, cases, heads, shape, qs, kvs):
    rows, cols, _ = shape
    tokens = rows * cols
    out_shape = [
        partial_shape(heads, tokens)
        if p
        else jax.ShapeDtypeStruct((heads * HDIM + STATS, tokens), jnp.float32)
        for p in packed
    ]
    return pl.pallas_call(
        functools.partial(attend_kernel, heads, tokens, cols, sets, packed, cases),
        out_shape=out_shape,
        in_specs=[WHOLE] * (len(qs) + len(kvs)),
        out_specs=[WHOLE] * len(packed),
        compiler_params=pltpu.CompilerParams(vmem_limit_bytes=16 * 2**20),
        cost_estimate=pl.CostEstimate(
            flops=10**9, bytes_accessed=8 * heads * tokens * HDIM, transcendentals=0
        ),
        name="attend",
    )(*qs, *kvs)


def merged(heads, tokens, ok_ref, local, priors, checks, write):
    lses = [local[heads * HDIM :, :]]
    for ref, flag in zip(priors, checks):
        ok = jnp.concatenate([ok_ref[flag : flag + 1, :]] * (tokens // HDIM), axis=1)
        lses.append(jnp.where(ok > 0, read_lse(ref, heads, tokens), NEVER))
    top = functools.reduce(jnp.maximum, lses)
    shares = [jnp.exp2(lse - top) for lse in lses]
    total = functools.reduce(jnp.add, shares)
    shares = [share * (1.0 / total) for share in shares]
    for j in range(heads):
        out = local[j * HDIM : (j + 1) * HDIM, :] * shares[0][j : j + 1, :]
        for ref, share in zip(priors, shares[1:]):
            piece = side_by_side(ref, j * tokens, tokens).astype(jnp.float32)
            out = out + piece * share[j : j + 1, :]
        write(j, out.astype(jnp.bfloat16))


def finish_kernel(heads, tokens, cols, first, checks, ok_ref, local, *refs):
    priors = refs[: len(checks)]
    out_ref, stage, sems = refs[-3:]
    copies = []

    def write(j, out):
        at = pl.ds(j * tokens, tokens)
        stage[at, :] = out.T
        copy = pltpu.make_async_copy(
            stage.at[at].reshape(tokens // cols, cols, HDIM),
            out_ref.at[0, :, :, pl.ds((first + j) * HDIM, HDIM)],
            sems.at[j],
        )
        copy.start()
        copies.append(copy)

    merged(heads, tokens, ok_ref, local, priors, checks, write)
    for copy in copies:
        copy.wait()


def finish(heads, shape, ok, first, local, priors, checks, into=None):
    rows, cols, channels = shape
    tokens = rows * cols
    args, aliases = [ok, local, *priors], {}
    specs = [WHOLE] * len(args)
    if into is not None:
        aliases = {len(args): 0}
        args.append(into)
        specs.append(pl.BlockSpec(memory_space=pl.ANY))
    return pl.pallas_call(
        functools.partial(finish_kernel, heads, tokens, cols, first, checks),
        out_shape=jax.ShapeDtypeStruct((1, rows, cols, channels), jnp.bfloat16),
        in_specs=specs,
        out_specs=pl.BlockSpec(memory_space=pl.ANY),
        input_output_aliases=aliases,
        scratch_shapes=[
            pltpu.VMEM((heads * tokens, HDIM), jnp.bfloat16),
            pltpu.SemaphoreType.DMA((heads,)),
        ],
        compiler_params=pltpu.CompilerParams(vmem_limit_bytes=8 * 2**20),
        cost_estimate=pl.CostEstimate(
            flops=10**8, bytes_accessed=8 * heads * tokens * HDIM, transcendentals=0
        ),
        name="finish",
    )(*args)


def steps(queries, keys, values, window):
    _, rows, cols, channels = queries.shape
    args = (
        pltpu.with_memory_space_constraint(a, pltpu.HBM) for a in (queries, keys, values, window)
    )
    half = channels // HDIM // 2
    shape = (rows, cols, channels)
    go = functools.partial(attend, heads=half, shape=shape)
    qa, kva, qb, kvb, ok = pack(half, *args)

    a1 = shift(kva, "tm", 1)
    a2 = shift(a1, "tm", 1, skip=1)
    qm = shift(qa, "space", 1)
    qp = shift(qa, "space", -1)
    along = (kva, a1, a2)
    frames = [tuple(3 * back + dy for back in range(3)) for dy in range(3)]
    both, mine = (True, True), (False,)
    first, second, edge = ("tm", 0), ("tm", 1), ("space", 0)
    pair_cases = (
        ((first, edge), (1,), (0,)),
        ((first,), (0, 1), (0,)),
        ((second, edge), (1,), (0, 1)),
        ((second,), (0, 1), (0, 1)),
    )
    frame_cases = (((first,), (0,), (0,)), ((second,), (0,), (0, 1)))
    km, kp = go((frames[2], frames[0]), both, pair_cases, qs=(qm, qp), kvs=along)
    pp = shift(km, "space", -1)
    pm = shift(kp, "space", 1)
    (ka,) = go((frames[1],), mine, frame_cases, qs=(qa,), kvs=along)

    grid = ("tm", "space")
    below = (1, 0)
    q1 = hop(qb, grid, (-1, 0), lambda place: place != below)
    q1_late = hop(qb, grid, (-1, 0), lambda place: place == below)
    hi = shift(kvb, "space", -1)
    q2 = shift(q1, "tm", -1, ahead=1)
    lo = shift(kvb, "space", 1)
    across = (lo, kvb, hi)
    offsets = [tuple(3 * back + dy for dy in range(3)) for back in range(3)]

    def row_cases(late=0):
        return (
            ((first, edge), (late,), (1, 2)),
            ((edge,), (0,), (1, 2)),
            ((("space", -1),), (0,), (0, 1)),
            ((), (0,), (0, 1, 2)),
        )

    (k2,) = go((offsets[2],), (True,), row_cases(), qs=(q2,), kvs=across)
    p2 = shift(k2, "tm", 2)
    (k1,) = go((offsets[1],) * 2, (True,), row_cases(1), qs=(q1, q1_late), kvs=across)
    p1 = shift(k1, "tm", 1)
    (k0,) = go((offsets[0],), mine, row_cases(), qs=(qb,), kvs=across)

    out = finish(half, shape, ok, half, k0, (p1, p2), (FRAME_1, FRAME_2))
    return finish(half, shape, ok, 0, ka, (pm, pp), (ROW_BEFORE, ROW_AFTER), into=out)


def solution(mesh):
    arrays = P(("group", "tm"), "space", None, "head")
    return jax.shard_map(
        steps,
        mesh=mesh,
        in_specs=(arrays, arrays, arrays, P(("group", "tm"), "space", None, None)),
        out_specs=arrays,
        check_vma=False,
    )
```
